32 devices in a mesh: patch: 16 (over z, y, x), pix: 2 (over core).
Axes of the slice: x: 2, y: 2, z: 4, core: 2. Of those that a mesh axis runs over, the one named last changes fastest.
Arguments:
- pixel_pos: float32 [2, 3072], P(None, ('patch', 'pix')), may hold values from -4 to 4
- pixel_view: float32 [3, 3072], P(None, ('patch', 'pix')), may hold values from -1 to 1
- observed: float32 [3072], P(('patch', 'pix')), may hold values from -6 to 6
- noise_scale: float32 [3072], P(('patch', 'pix')), may hold values from 0.5 to 2
- valid_mask: int32 [3072], P(('patch', 'pix')), may hold values 0 or 1
- patch_pos: float32 [2, 768], P(None, 'patch'), may hold values from -4 to 4
- patch_depth: float32 [768], P('patch'), may hold values from 0.3 to 1.5
- segment_ids: int32 [768], P('patch'), may hold values from 0 to 15, never falling along the last dimension, each value on 1 to 192 neighbouring positions
- seg_strike: float32 [16], replicated, may hold values from -3.140625 to 3.140625
- seg_dip: float32 [16], replicated, may hold values from 0.35 to 1.4
- slip_models: bfloat16 [768, 3, 128], P('patch'), may hold values from -0.8984375 to 0.8984375
Outputs:
- residual: float32 [3072, 128], P(('patch', 'pix'))
- misfit: float32 [128], replicated
The draws below stay inside these ranges and needn't reach their ends.
Inputs may be any that keep to these rules, and one draw needn't show every extreme that they name: `segment_ids`: segment ids never fall along the patches.
All inputs are finite; a program needn't handle non-finite values. No bound on the sum of `valid_mask` on one device may be relied on, other than what follows from the above.
Results may differ from the reference program's by a relative error of at most 0.0003.
Values may be sent and summed in bfloat16 or wider, within the bound.
A program may use at most 64 MiB of HBM per device.

```python
import math
import jax
import jax.numpy as jnp
import numpy as np
from jax import lax

PATCH_DEV = 48
SAMPLES = 128
SEGMENTS = 16
PATCHES = 768
PIXELS = 3072
N_PATCH = 16


def touch_ends(values, rng, least, top_value):
    spot = [jax.random.randint(jax.random.fold_in(rng, axis), (), 0, length) for axis, length in enumerate(values.shape)]
    longest = values.shape.index(max(values.shape))
    neighbour = spot[:longest] + [(spot[longest] + 1) % values.shape[longest]] + spot[longest + 1:]
    return values.at[tuple(spot)].set(least).at[tuple(neighbour)].set(top_value)


def block_scale(own_key, dims, shards, smallest, top_value):
    def one(dim, parts):
        draws = jax.random.uniform(jax.random.fold_in(jax.random.fold_in(own_key, 6), dim), (parts,), jnp.float32, smallest / len(shards), top_value / len(shards))
        return jnp.repeat(jnp.exp(draws), dims[dim] // parts).reshape((-1,) + (1,) * (len(dims) - dim - 1))

    loudness = one(*shards[0])
    for cut in shards[1:]:
        loudness = loudness * one(*cut)
    return loudness


def split_up(number_of, total, most, slope):
    portions = [(1 << 20) // math.isqrt(standing ** slope) + 1 for standing in range(2, number_of + 1)]
    surplus, counts = total - most - (number_of - 1), [1] * (number_of - 1)
    while surplus > 0:
        candidates = [i for i in range(number_of - 1) if counts[i] < most]
        mass, remaining = sum([portions[i] for i in candidates]), surplus
        for i in candidates:
            more = min(most - counts[i], max(1, remaining * portions[i] // mass), surplus)
            counts[i] = counts[i] + more
            surplus = surplus - more
    return np.array([most] + counts)


def ragged_sizes(own_key, count, total, most, skew):
    if count == 2:
        one = jax.random.randint(own_key, (), max(1, total - most), min(most, total - 1) + 1)
        return jnp.stack([one, total - one])
    tallies = jnp.asarray(split_up(count, total, most, skew), jnp.int32)
    couples = (count - 1) // 2
    source_of, receiver = tallies[1:1 + 2 * couples:2], tallies[2:2 + 2 * couples:2]
    room = jnp.minimum(source_of - 1, most - receiver)
    shifted = jax.random.randint(jax.random.fold_in(own_key, 1), (couples,), 0, 1 << 20) % (room + 1)
    tallies = tallies.at[1:1 + 2 * couples:2].set(source_of - shifted).at[2:2 + 2 * couples:2].set(receiver + shifted)
    return tallies[jax.random.permutation(jax.random.fold_in(own_key, 2), count)]


def normal_values(own_key, dims, spread, bound, shards=(), kind=jnp.bfloat16):
    array = jax.random.normal(own_key, dims, jnp.float32) * spread
    if len(shards) > 0:
        array = block_scale(own_key, dims, shards, -0.22, 0.18) * array
    return jnp.clip(array, min=-bound, max=bound).astype(kind)


def setup_inputs(seed: int = 0) -> dict:
    keys = jax.random.split(jax.random.key(seed), 12)
    pixel_pos = jnp.clip(jax.random.uniform(keys[0], (2, PIXELS), jnp.float32, -4.0, 4.0) * block_scale(keys[0], (2, PIXELS), ((1, 32),), -0.4, 0.0), -4.0, 4.0)
    pixel_view = jnp.clip(jax.random.uniform(keys[1], (3, PIXELS), jnp.float32, -1.0, 1.0) * block_scale(keys[1], (3, PIXELS), ((1, 32),), -0.4, 0.0), -1.0, 1.0)
    observed = normal_values(keys[2], (PIXELS,), 1.0, 6.0, ((0, 32),), jnp.float32)
    noise_scale = jnp.clip(jnp.exp(math.log(2.0) - 1.3862944 * jax.random.uniform(keys[3], (PIXELS,), jnp.float32) ** block_scale(keys[3], (PIXELS,), ((0, 32),), -0.2, 0.2)), 0.5, 2.0)
    valid_mask = touch_ends((jax.random.randint(keys[4], (PIXELS,), 0, 8) < 7).astype(jnp.int32), jax.random.fold_in(keys[4], 1), 0, 1)
    patch_pos = jnp.clip(jax.random.uniform(keys[5], (2, PATCHES), jnp.float32, -4.0, 4.0) * block_scale(keys[5], (2, PATCHES), ((1, 16),), -0.4, 0.0), -4.0, 4.0)
    patch_depth = jnp.clip(0.3 + 1.2 * jax.random.uniform(keys[6], (PATCHES,), jnp.float32) ** block_scale(keys[6], (PATCHES,), ((0, 16),), -0.2, 0.2), 0.3, 1.5)
    segment_ids = jnp.searchsorted(jnp.cumsum(ragged_sizes(keys[7], SEGMENTS, PATCHES, PATCH_DEV * N_PATCH // 4, 1)), jnp.arange(PATCHES), side="right").astype(jnp.int32)
    seg_strike = jnp.clip(jax.random.uniform(keys[8], (SEGMENTS,), jnp.float32, -3.140625, 3.140625), -3.140625, 3.140625)
    seg_dip = jnp.clip(jax.random.uniform(keys[9], (SEGMENTS,), jnp.float32, 0.35, 1.4), 0.35, 1.4)
    slip_models = normal_values(keys[10], (PATCHES, 3, SAMPLES), 0.15, 0.8984375, ((0, 16),))
    return {"pixel_pos": pixel_pos, "pixel_view": pixel_view, "observed": observed, "noise_scale": noise_scale, "valid_mask": valid_mask, "patch_pos": patch_pos, "patch_depth": patch_depth, "segment_ids": segment_ids, "seg_strike": seg_strike, "seg_dip": seg_dip, "slip_models": slip_models}


two_pi = 2.0 * math.pi
mu_ratio = 0.5

def point_green(pixel_pos, pixel_view, frame_rows):
    src_east = frame_rows[0][:, None]
    src_north = frame_rows[1][:, None]
    src_depth = frame_rows[2][:, None]
    sin_strike = frame_rows[3][:, None]
    cos_strike = frame_rows[4][:, None]
    sin_dip = frame_rows[5][:, None]
    cos_dip = frame_rows[6][:, None]
    east_gap = pixel_pos[0][None, :] - src_east
    north_gap = pixel_pos[1][None, :] - src_north
    along_x = east_gap * sin_strike + north_gap * cos_strike
    across = north_gap * sin_strike - east_gap * cos_strike
    depth_term = across * cos_dip + src_depth * sin_dip
    plane_term = across * sin_dip - src_depth * cos_dip
    radius = jnp.sqrt(along_x * along_x + across * across + src_depth * src_depth)
    over_r = 1.0 / radius
    over_r3 = over_r * over_r * over_r
    over_r5 = over_r3 * over_r * over_r
    over_rd = 1.0 / (radius + src_depth)
    base_term = over_r * over_rd * over_rd
    cubic_term = (3.0 * radius + src_depth) * over_r3 * over_rd * over_rd * over_rd
    square_term = (2.0 * radius + src_depth) * over_r3 * over_rd * over_rd
    term_one = mu_ratio * across * (base_term - along_x * along_x * cubic_term)
    term_two = mu_ratio * along_x * (base_term - across * across * cubic_term)
    term_three = mu_ratio * along_x * over_r3 - term_two
    term_four = -mu_ratio * along_x * across * square_term
    term_five = mu_ratio * (over_r * over_rd - along_x * along_x * square_term)
    scaled_q = 3.0 * plane_term * over_r5
    dip_mixed = sin_dip * cos_dip
    dip_square = sin_dip * sin_dip
    strike_x = -(scaled_q * along_x * along_x + term_one * sin_dip)
    strike_y = -(scaled_q * along_x * across + term_two * sin_dip)
    strike_z = -(scaled_q * along_x * src_depth + term_four * sin_dip)
    dip_x = -(scaled_q * along_x * depth_term - term_three * dip_mixed)
    dip_y = -(scaled_q * across * depth_term - term_one * dip_mixed)
    dip_z = -(scaled_q * src_depth * depth_term - term_five * dip_mixed)
    open_x = scaled_q * along_x * plane_term - term_three * dip_square
    open_y = scaled_q * across * plane_term - term_one * dip_square
    open_z = scaled_q * src_depth * plane_term - term_five * dip_square

    def project(comp_x, comp_y, comp_z):
        east_move = comp_x * sin_strike - comp_y * cos_strike
        north_move = comp_x * cos_strike + comp_y * sin_strike
        return (pixel_view[0][None, :] * east_move + pixel_view[1][None, :] * north_move + pixel_view[2][None, :] * comp_z) / two_pi
    return jnp.stack([project(strike_x, strike_y, strike_z), project(dip_x, dip_y, dip_z), project(open_x, open_y, open_z)], axis=1)

def reference(pixel_pos, pixel_view, observed, noise_scale, valid_mask, patch_pos, patch_depth, segment_ids, seg_strike, seg_dip, slip_models):
    strike = jnp.take(seg_strike, segment_ids)
    dip_angle = jnp.take(seg_dip, segment_ids)
    frames = jnp.stack([patch_pos[0], patch_pos[1], patch_depth, jnp.sin(strike), jnp.cos(strike), jnp.sin(dip_angle), jnp.cos(dip_angle)], axis=0)
    patch_count = patch_depth.shape[0]
    block_size = math.gcd(patch_count, 64)
    block_count = patch_count // block_size
    samples = slip_models.shape[2]
    framed = frames.reshape(7, block_count, block_size).transpose(1, 0, 2)
    slip_blocks = slip_models.reshape(block_count, block_size * 3, samples)

    def add_block(running, block_items):
        frame_rows, block_slip = block_items
        green_tile = point_green(pixel_pos, pixel_view, frame_rows).astype(jnp.bfloat16)
        green_tile = lax.optimization_barrier(green_tile).reshape(block_size * 3, PIXELS)
        part_sum = lax.dot_general(green_tile.astype(jnp.float32), block_slip.astype(jnp.float32), (((0,), (0,)), ((), ())), precision=lax.Precision.HIGHEST)
        return (running + part_sum, None)
    predicted, _ = lax.scan(add_block, jnp.zeros((PIXELS, samples), jnp.float32), (framed, slip_blocks))
    residual = valid_mask.astype(jnp.float32)[:, None] * (predicted - observed[:, None]) / noise_scale[:, None]
    misfit = lax.optimization_barrier(jnp.sum(residual * residual, axis=0)) / PIXELS
    return (residual, misfit)
```

```python
import functools
import math

import jax
import jax.numpy as jnp
from jax import lax
from jax.experimental import pallas as pl
from jax.experimental.pallas import tpu as pltpu
from jax.sharding import PartitionSpec as P

MESH = pl.DeviceIdType.MESH
inv_two_pi = 1.0 / (2.0 * math.pi)
mu_ratio = 0.5
LANES = 128


def green_rows(sites, columns):
    src_east, src_north, depth, sin_s, cos_s, sin_d, cos_d = columns
    view_up = sites[4:5]
    east = sites[0:1] - src_east
    north = sites[1:2] - src_north
    x = east * sin_s + north * cos_s
    y = north * sin_s - east * cos_s
    view_x = sites[2:3] * sin_s + sites[3:4] * cos_s
    view_y = sites[3:4] * sin_s - sites[2:3] * cos_s
    p = y * cos_d + depth * sin_d
    q = y * sin_d - depth * cos_d
    xx = x * x
    yy = y * y
    rr = xx + yy + depth * depth
    over_r = lax.rsqrt(rr)
    radius = rr * over_r
    over_rd = 1.0 / (radius + depth)
    a = over_r * over_rd
    aa = a * a
    base = a * over_rd
    cubic = (3.0 * radius + depth) * (aa * a)
    square = (2.0 * radius + depth) * (aa * over_r)
    over_r2 = over_r * over_r
    over_r3 = over_r2 * over_r
    one = y * (base - xx * cubic)
    two = x * (base - yy * cubic)
    three = x * over_r3 - two
    four = x * y * square
    five = a - xx * square
    look = x * view_x + y * view_y + depth * view_up
    t = 3.0 * q * (over_r3 * over_r2) * look
    line_one = one * view_x + two * view_y - four * view_up
    line_two = three * view_x + one * view_y + five * view_up
    half_sin = mu_ratio * sin_d
    return (
        -(t * x + half_sin * line_one),
        half_sin * cos_d * line_two - t * p,
        t * q - half_sin * sin_d * line_two,
    )


def kernel(
    n,
    sites_ref,
    frames_ref,
    slip_ref,
    stats_ref,
    residual_ref,
    misfit_ref,
    sites_in,
    frames_in,
    slips_in,
    acc,
    part_in,
    sums_in,
    group_send,
    fwd_send,
    recv_sem,
    pair_send,
    pair_recv,
    sums_send,
    sums_recv,
):
    me = lax.axis_index("patch")
    core = lax.axis_index("pix")
    half = n // 2
    count = 2 * n
    rank = me * 2 + core
    parity = lax.rem(me, 2)
    place = me // 2
    across = me + 1 - 2 * parity
    sibling = 1 - core
    width = slip_ref.shape[0] // 3

    barrier = pltpu.get_barrier_semaphore()

    @pl.loop(1, count)
    def _(t):
        peer = lax.rem(rank + t, count)
        pl.semaphore_signal(
            barrier, inc=1, device_id=(peer // 2, lax.rem(peer, 2)), device_id_type=MESH
        )

    pl.semaphore_wait(barrier, count - 1)

    def remote(src, dst, send, recv, target):
        return pltpu.make_async_remote_copy(
            src_ref=src,
            dst_ref=dst,
            send_sem=send,
            recv_sem=recv,
            device_id=target,
            device_id_type=MESH,
        )

    def block_copies(frames, slip, slot, sends, step, target):
        return (
            remote(frames, frames_in.at[slot], sends.at[0, step], recv_sem.at[0, slot], target),
            remote(slip, slips_in.at[slot], sends.at[1, step], recv_sem.at[1, slot], target),
        )

    def group_member(t):
        return parity + 2 * lax.rem(place + t, half)

    own_across = block_copies(frames_ref, slip_ref, me, fwd_send, 0, (across, core))
    sites_copy = remote(sites_ref, sites_in, pair_send.at[0], pair_recv.at[0], (me, sibling))
    sites_copy.start()
    for copy in own_across:
        copy.start()

    @pl.loop(1, half)
    def _(t):
        for copy in block_copies(frames_ref, slip_ref, me, group_send, t, (group_member(t), core)):
            copy.start()

    acc[...] = jnp.zeros_like(acc)
    sites_copy.wait_recv()

    def add_source(frames, slip):
        turned = frames.T
        columns = [turned[:width, k : k + 1] for k in range(7)]
        for side, ref in enumerate((sites_ref, sites_in)):
            rows = jnp.concatenate(green_rows(ref[...], columns), axis=0)
            acc[side] += lax.dot_general(
                slip,
                rows.astype(jnp.bfloat16),
                (((0,), (0,)), ((), ())),
                preferred_element_type=jnp.float32,
            )

    add_source(frames_ref[...], slip_ref[...])

    @pl.loop(1, half)
    def _(t):
        source = group_member(half - t)
        incoming = block_copies(frames_ref, slip_ref, source, group_send, t, (across, core))
        onward = block_copies(
            frames_in.at[source], slips_in.at[source], source, fwd_send, t, (across, core)
        )
        for get, put in zip(incoming, onward):
            get.wait_recv()
            put.start()
        add_source(frames_in[source], slips_in[source])

    @pl.loop(0, half)
    def _(t):
        source = 1 - parity + 2 * lax.rem(place + half - t, half)
        for get in block_copies(frames_ref, slip_ref, source, group_send, 0, (across, core)):
            get.wait_recv()
        add_source(frames_in[source], slips_in[source])

    part_copy = remote(acc.at[1], part_in, pair_send.at[1], pair_recv.at[1], (me, sibling))
    part_copy.start()
    part_copy.wait_recv()
    observed, noise, valid = stats_ref[0:1], stats_ref[1:2], stats_ref[2:3]
    scaled = valid * (acc[0] + part_in[...] - observed) / noise
    residual = scaled.T[: residual_ref.shape[0]]
    sums_in[rank] = jnp.sum(residual * residual, axis=0, keepdims=True)

    @pl.loop(1, count)
    def _(t):
        peer = lax.rem(rank + t, count)
        remote(
            sums_in.at[rank],
            sums_in.at[rank],
            sums_send.at[t],
            sums_recv.at[rank],
            (peer // 2, lax.rem(peer, 2)),
        ).start()

    residual_ref[...] = residual

    sites_copy.wait_send()
    part_copy.wait_send()
    for copy in own_across:
        copy.wait_send()

    @pl.loop(1, half)
    def _(t):
        for copy in block_copies(frames_ref, slip_ref, me, group_send, t, (group_member(t), core)):
            copy.wait_send()
        source = group_member(half - t)
        for copy in block_copies(
            frames_in.at[source], slips_in.at[source], source, fwd_send, t, (across, core)
        ):
            copy.wait_send()

    @pl.loop(1, count)
    def _(t):
        peer = lax.rem(rank + t, count)
        target = (peer // 2, lax.rem(peer, 2))
        remote(
            sums_in.at[rank], sums_in.at[rank], sums_send.at[t], sums_recv.at[rank], target
        ).wait_send()
        remote(
            sums_in.at[rank], sums_in.at[peer], sums_send.at[t], sums_recv.at[peer], target
        ).wait_recv()

    pixels = residual_ref.shape[0] * count
    misfit_ref[...] = jnp.sum(sums_in[...], axis=0) / pixels


def padded(rows):
    table = jnp.stack(rows, axis=0)
    return jnp.pad(table, ((0, 8 - table.shape[0]), (0, LANES - table.shape[1])))


def per_device(
    n,
    pixel_pos,
    pixel_view,
    observed,
    noise_scale,
    valid_mask,
    patch_pos,
    patch_depth,
    segment_ids,
    seg_strike,
    seg_dip,
    slip_models,
):
    own_pixels = pixel_pos.shape[1]
    samples = slip_models.shape[2]
    width = slip_models.shape[0] // 2
    start = lax.axis_index("pix") * width
    view = pixel_view * inv_two_pi
    sites = padded([pixel_pos[0], pixel_pos[1], view[0], view[1], view[2]])
    mask = valid_mask.astype(jnp.float32)
    stats = jnp.pad(
        jnp.stack([observed, noise_scale, mask], axis=0), ((0, 5), (0, LANES - own_pixels))
    )
    stats = stats.at[1, own_pixels:].set(1.0)
    segments = seg_strike.shape[0]
    matches = segment_ids[:, None] == jnp.arange(segments, dtype=jnp.int32)[None, :]
    strike = jnp.sum(jnp.where(matches, seg_strike[None, :], 0.0), axis=1)
    dip = jnp.sum(jnp.where(matches, seg_dip[None, :], 0.0), axis=1)
    rows = [patch_pos[0], patch_pos[1], patch_depth]
    rows += [jnp.sin(strike), jnp.cos(strike), jnp.sin(dip), jnp.cos(dip)]
    frames = lax.dynamic_slice_in_dim(jnp.stack(rows, axis=0), start, width, axis=1)
    frames = jnp.pad(frames, ((0, 1), (0, LANES - width)))
    slip = lax.dynamic_slice_in_dim(slip_models, start, width, axis=0)
    slip = slip.transpose(1, 0, 2).reshape(3 * width, samples)
    half = n // 2
    vmem = pl.BlockSpec(memory_space=pltpu.VMEM)
    residual, misfit = pl.pallas_call(
        functools.partial(kernel, n),
        out_shape=(
            jax.ShapeDtypeStruct((own_pixels, samples), jnp.float32),
            jax.ShapeDtypeStruct((1, samples), jnp.float32),
        ),
        in_specs=[vmem] * 4,
        out_specs=(vmem, vmem),
        scratch_shapes=[
            pltpu.VMEM((8, LANES), jnp.float32),
            pltpu.VMEM((n, 8, LANES), jnp.float32),
            pltpu.VMEM((n, 3 * width, samples), jnp.bfloat16),
            pltpu.VMEM((2, samples, LANES), jnp.float32),
            pltpu.VMEM((samples, LANES), jnp.float32),
            pltpu.VMEM((2 * n, 1, samples), jnp.float32),
            pltpu.SemaphoreType.DMA((2, half)),
            pltpu.SemaphoreType.DMA((2, half)),
            pltpu.SemaphoreType.DMA((2, n)),
            pltpu.SemaphoreType.DMA((2,)),
            pltpu.SemaphoreType.DMA((2,)),
            pltpu.SemaphoreType.DMA((2 * n,)),
            pltpu.SemaphoreType.DMA((2 * n,)),
        ],
        compiler_params=pltpu.CompilerParams(collective_id=0, has_side_effects=True),
    )(sites, frames, slip, stats)
    return residual, misfit.reshape(samples)


def solution(mesh):
    return jax.shard_map(
        functools.partial(per_device, mesh.shape["patch"]),
        mesh=mesh,
        in_specs=(
            P(None, ("patch", "pix")),
            P(None, ("patch", "pix")),
            P(("patch", "pix")),
            P(("patch", "pix")),
            P(("patch", "pix")),
            P(None, "patch"),
            P("patch"),
            P("patch"),
            P(),
            P(),
            P("patch", None, None),
        ),
        out_specs=(P(("patch", "pix"), None), P()),
        check_vma=False,
    )
```

```python
import functools
import math

import jax
import jax.numpy as jnp
from jax import lax
from jax.experimental import pallas as pl
from jax.experimental.pallas import tpu as pltpu
from jax.sharding import PartitionSpec as P

MESH = pl.DeviceIdType.MESH
inv_two_pi = 1.0 / (2.0 * math.pi)
mu_ratio = 0.5
LANES = 128


def green_rows(sites, columns):
    src_east, src_north, depth, sin_s, cos_s, sin_d, cos_d = columns
    view_up = sites[4:5]
    east = sites[0:1] - src_east
    north = sites[1:2] - src_north
    x = east * sin_s + north * cos_s
    y = north * sin_s - east * cos_s
    view_x = sites[2:3] * sin_s + sites[3:4] * cos_s
    view_y = sites[3:4] * sin_s - sites[2:3] * cos_s
    p = y * cos_d + depth * sin_d
    q = y * sin_d - depth * cos_d
    xx = x * x
    yy = y * y
    rr = xx + yy + depth * depth
    over_r = lax.rsqrt(rr)
    radius = rr * over_r
    over_rd = 1.0 / (radius + depth)
    a = over_r * over_rd
    aa = a * a
    base = a * over_rd
    cubic = (3.0 * radius + depth) * (aa * a)
    square = (2.0 * radius + depth) * (aa * over_r)
    over_r2 = over_r * over_r
    over_r3 = over_r2 * over_r
    one = y * (base - xx * cubic)
    two = x * (base - yy * cubic)
    three = x * over_r3 - two
    four = x * y * square
    five = a - xx * square
    look = x * view_x + y * view_y + depth * view_up
    t = 3.0 * q * (over_r3 * over_r2) * look
    line_one = one * view_x + two * view_y - four * view_up
    line_two = three * view_x + one * view_y + five * view_up
    half_sin = mu_ratio * sin_d
    return (
        -(t * x + half_sin * line_one),
        half_sin * cos_d * line_two - t * p,
        t * q - half_sin * sin_d * line_two,
    )


def frame_table(core, pos, depth, ids, strike, dip, width):
    segments = strike.shape[1]
    rows = lax.broadcasted_iota(jnp.int32, (segments, segments), 0)
    diagonal = rows == lax.broadcasted_iota(jnp.int32, (segments, segments), 1)
    matches = lax.broadcasted_iota(jnp.int32, (segments, ids.shape[1]), 0) == ids

    def lookup(row):
        column = jnp.sum(jnp.where(diagonal, row, 0.0), axis=1, keepdims=True)
        return jnp.sum(jnp.where(matches, column, 0.0), axis=0, keepdims=True)

    angles = jnp.concatenate([lookup(strike), lookup(dip)], axis=0)
    sines, cosines = jnp.sin(angles), jnp.cos(angles)
    table = jnp.concatenate([pos, depth, sines[0:1], cosines[0:1], sines[1:2], cosines[1:2]], axis=0)
    table = jnp.where(core == 1, table[:, width:], table[:, :width])
    table = jnp.concatenate([table, jnp.zeros((7, LANES // 4 - width), jnp.float32)], axis=1)
    spare = jnp.zeros((1, LANES // 4), jnp.float32)
    upper = jnp.concatenate([table[k : k + 1] for k in range(4)], axis=1)
    lower = jnp.concatenate([table[k : k + 1] for k in range(4, 7)] + [spare], axis=1)
    return jnp.concatenate([upper, lower], axis=0)


def kernel(
    n,
    *refs,
):
    args, refs = refs[:11], refs[11:]
    residual_ref, misfit_ref, refs = refs[0], refs[1], refs[2:]
    local, refs = refs[:11], refs[11:]
    (
        sites_own,
        sites_in,
        frames_in,
        slips_in,
        greens,
        acc,
        part_in,
        sums_in,
        load_sem,
        frames_send,
        frames_recv,
        group_send,
        fwd_send,
        slip_recv,
        pair_send,
        pair_recv,
        sums_send,
        sums_recv,
    ) = refs
    me = lax.axis_index("patch")
    core = lax.axis_index("pix")
    half = n // 2
    count = 2 * n
    rank = me * 2 + core
    parity = lax.rem(me, 2)
    place = me // 2
    across = me + 1 - 2 * parity
    sibling = 1 - core
    width = local[10].shape[1]
    pixels = residual_ref.shape[0]

    barrier = pltpu.get_barrier_semaphore()

    @pl.loop(1, count)
    def _(t):
        peer = lax.rem(rank + t, count)
        pl.semaphore_signal(
            barrier, inc=1, device_id=(peer // 2, lax.rem(peer, 2)), device_id_type=MESH
        )

    loads = []
    for k in range(11):
        src = args[k]
        if k == 10:
            src = src.at[:, pl.ds(pl.multiple_of(core * width, 8), width)]
        loads.append(pltpu.make_async_copy(src, local[k], load_sem.at[k]))
    for load in loads:
        load.start()
    for load in loads:
        load.wait()

    sites_own[...] = jnp.zeros_like(sites_own)
    sites_own[0:2, :pixels] = local[0][...]
    sites_own[2:5, :pixels] = local[1][...] * inv_two_pi
    frames_in[me] = frame_table(core, *[local[k][...] for k in range(5, 10)], width)
    slip = local[10][...].astype(jnp.float32)
    rows = [slip[k] for k in range(3)] + [jnp.zeros((8, slip.shape[2]), jnp.float32)]
    slips_in[0, place] = jnp.concatenate(rows, axis=0).astype(jnp.bfloat16)

    pl.semaphore_wait(barrier, count - 1)

    def remote(src, dst, send, recv, target):
        return pltpu.make_async_remote_copy(
            src_ref=src,
            dst_ref=dst,
            send_sem=send,
            recv_sem=recv,
            device_id=target,
            device_id_type=MESH,
        )

    def frames_copy(t):
        source, target = me, lax.rem(me + t, n)
        return remote(
            frames_in.at[source],
            frames_in.at[source],
            frames_send.at[t],
            frames_recv.at[source],
            (target, core),
        )

    def group_copy(t):
        target = parity + 2 * lax.rem(place + t, half)
        mine = slips_in.at[0, place]
        return remote(mine, mine, group_send.at[t], slip_recv.at[0, place], (target, core))

    def onward_copy(slot):
        return remote(
            slips_in.at[0, slot],
            slips_in.at[1, slot],
            fwd_send.at[slot],
            slip_recv.at[1, slot],
            (across, core),
        )

    def arrival(ref, sem):
        return remote(ref, ref, pair_send.at[0], sem, (across, core))

    sites_copy = remote(sites_own, sites_in, pair_send.at[0], pair_recv.at[0], (me, sibling))
    sites_copy.start()

    @pl.loop(1, n)
    def _(t):
        frames_copy(t).start()

    onward_copy(place).start()

    @pl.loop(1, half)
    def _(t):
        group_copy(t).start()

    def add_green(side, slot):
        source = 2 * slot + (parity if side == 0 else 1 - parity)
        turned = jnp.concatenate([frames_in[source], jnp.zeros((6, LANES), jnp.float32)], axis=0).T
        columns = []
        for k in range(7):
            base = (k % 4) * (LANES // 4)
            columns.append(turned[base : base + width, k // 4 : k // 4 + 1])
        for lane, ref in enumerate((sites_own, sites_in)):
            rows = green_rows(ref[...], columns) + (jnp.zeros((8, LANES), jnp.float32),)
            block = jnp.concatenate(rows, axis=0).astype(jnp.bfloat16)
            greens[side, slot, :, lane * LANES : (lane + 1) * LANES] = block

    def wait_frames(side, slot):
        source = 2 * slot + (parity if side == 0 else 1 - parity)
        arrival(frames_in.at[source], frames_recv.at[source]).wait_recv()

    sites_copy.wait_recv()
    add_green(0, place)

    @pl.loop(1, half)
    def _(t):
        slot = lax.rem(place + half - t, half)
        wait_frames(0, slot)
        add_green(0, slot)
        arrival(slips_in.at[0, slot], slip_recv.at[0, slot]).wait_recv()
        onward_copy(slot).start()
        wait_frames(1, slot)
        add_green(1, slot)

    wait_frames(1, place)
    add_green(1, place)

    chunk = math.gcd(half, 8)

    def product(side, step, lane):
        slips = slips_in[side, pl.ds(step * chunk, chunk)]
        block = greens[side, pl.ds(step * chunk, chunk), :, lane * LANES : (lane + 1) * LANES]
        return lax.dot_general(
            slips.reshape(-1, slips.shape[-1]),
            block.reshape(-1, LANES),
            (((0,), (0,)), ((), ())),
            preferred_element_type=jnp.float32,
        )

    acc[...] = jnp.zeros_like(acc)

    @pl.loop(0, half // chunk)
    def _(step):
        for lane in range(2):
            acc[lane] += product(0, step, lane)

    @pl.loop(0, half)
    def _(t):
        slot = lax.rem(place + half - t, half)
        arrival(slips_in.at[1, slot], slip_recv.at[1, slot]).wait_recv()

    @pl.loop(0, half // chunk)
    def _(step):
        acc[1] += product(1, step, 1)

    part_copy = remote(acc.at[1], part_in, pair_send.at[1], pair_recv.at[1], (me, sibling))
    part_copy.start()

    @pl.loop(0, half // chunk)
    def _(step):
        acc[0] += product(1, step, 0)

    valid = local[4][...].astype(jnp.float32)
    part_copy.wait_recv()
    total = (acc[0] + part_in[...])[:, :pixels]
    scaled = valid * (total - local[2][...]) / local[3][...]
    blank = jnp.zeros((total.shape[0], LANES - pixels), jnp.float32)
    residual = jnp.concatenate([scaled, blank], axis=1).T[:pixels]
    sums_in[rank] = jnp.sum(residual * residual, axis=0, keepdims=True)

    def sums_copy(t, slot):
        peer = lax.rem(rank + t, count)
        return remote(
            sums_in.at[slot],
            sums_in.at[slot],
            sums_send.at[t],
            sums_recv.at[slot],
            (peer // 2, lax.rem(peer, 2)),
        )

    @pl.loop(1, count)
    def _(t):
        sums_copy(t, rank).start()

    residual_ref[...] = residual
    sites_copy.wait_send()
    part_copy.wait_send()

    @pl.loop(1, n)
    def _(t):
        frames_copy(t).wait_send()

    @pl.loop(1, half)
    def _(t):
        group_copy(t).wait_send()

    @pl.loop(0, half)
    def _(slot):
        onward_copy(slot).wait_send()

    @pl.loop(1, count)
    def _(t):
        sums_copy(t, rank).wait_send()
        sums_copy(t, lax.rem(rank + t, count)).wait_recv()

    misfit_ref[...] = jnp.sum(sums_in[...], axis=0) / (pixels * count)


def per_device(n, *args):
    args = [arg.reshape(1, -1) if arg.ndim == 1 else arg for arg in args]
    args[10] = args[10].transpose(1, 0, 2)
    own_pixels = args[0].shape[1]
    width = args[10].shape[1] // 2
    samples = args[10].shape[2]
    half = n // 2
    vmem = pl.BlockSpec(memory_space=pltpu.VMEM)
    local = [pltpu.VMEM(arg.shape, arg.dtype) for arg in args[:10]]
    local.append(pltpu.VMEM((3, width, samples), jnp.bfloat16))
    depth = 3 * width + 8
    dma = pltpu.SemaphoreType.DMA
    residual, misfit = pl.pallas_call(
        functools.partial(kernel, n),
        out_shape=(
            pltpu.VMEM((own_pixels, samples), jnp.float32),
            pltpu.VMEM((1, samples), jnp.float32),
        ),
        in_specs=[pl.BlockSpec(memory_space=pl.ANY)] * 11,
        out_specs=(vmem, vmem),
        scratch_shapes=local
        + [
            pltpu.VMEM((8, LANES), jnp.float32),
            pltpu.VMEM((8, LANES), jnp.float32),
            pltpu.VMEM((n, 2, LANES), jnp.float32),
            pltpu.VMEM((2, half, depth, samples), jnp.bfloat16),
            pltpu.VMEM((2, half, depth, 2 * LANES), jnp.bfloat16),
            pltpu.VMEM((2, samples, LANES), jnp.float32),
            pltpu.VMEM((samples, LANES), jnp.float32),
            pltpu.VMEM((2 * n, 1, samples), jnp.float32),
            dma((11,)),
            dma((n,)),
            dma((n,)),
            dma((half,)),
            dma((half,)),
            dma((2, half)),
            dma((2,)),
            dma((2,)),
            dma((2 * n,)),
            dma((2 * n,)),
        ],
        compiler_params=pltpu.CompilerParams(collective_id=0, has_side_effects=True),
    )(*args)
    return residual, misfit.reshape(samples)


def solution(mesh):
    return jax.shard_map(
        functools.partial(per_device, mesh.shape["patch"]),
        mesh=mesh,
        in_specs=(
            P(None, ("patch", "pix")),
            P(None, ("patch", "pix")),
            P(("patch", "pix")),
            P(("patch", "pix")),
            P(("patch", "pix")),
            P(None, "patch"),
            P("patch"),
            P("patch"),
            P(),
            P(),
            P("patch", None, None),
        ),
        out_specs=(P(("patch", "pix"), None), P()),
        check_vma=False,
    )
```

```python
import functools
import math

import jax
import jax.numpy as jnp
from jax import lax
from jax.experimental import pallas as pl
from jax.experimental.pallas import tpu as pltpu
from jax.sharding import PartitionSpec as P

MESH = pl.DeviceIdType.MESH
inv_two_pi = 1.0 / (2.0 * math.pi)
mu_ratio = 0.5
LANES = 128


def green_rows(sites, columns):
    src_east, src_north, depth, sin_s, cos_s, sin_d, cos_d = columns
    view_up = sites[4:5]
    east = sites[0:1] - src_east
    north = sites[1:2] - src_north
    x = east * sin_s + north * cos_s
    y = north * sin_s - east * cos_s
    view_x = sites[2:3] * sin_s + sites[3:4] * cos_s
    view_y = sites[3:4] * sin_s - sites[2:3] * cos_s
    p = y * cos_d + depth * sin_d
    q = y * sin_d - depth * cos_d
    xx = x * x
    yy = y * y
    rr = xx + yy + depth * depth
    over_r = lax.rsqrt(rr)
    radius = rr * over_r
    over_rd = 1.0 / (radius + depth)
    a = over_r * over_rd
    aa = a * a
    base = a * over_rd
    cubic = (3.0 * radius + depth) * (aa * a)
    square = (2.0 * radius + depth) * (aa * over_r)
    over_r2 = over_r * over_r
    over_r3 = over_r2 * over_r
    one = y * (base - xx * cubic)
    two = x * (base - yy * cubic)
    three = x * over_r3 - two
    four = x * y * square
    five = a - xx * square
    look = x * view_x + y * view_y + depth * view_up
    t = 3.0 * q * (over_r3 * over_r2) * look
    line_one = one * view_x + two * view_y - four * view_up
    line_two = three * view_x + one * view_y + five * view_up
    half_sin = mu_ratio * sin_d
    return (
        -(t * x + half_sin * line_one),
        half_sin * cos_d * line_two - t * p,
        t * q - half_sin * sin_d * line_two,
    )


def frame_table(core, pos, depth, ids, strike, dip, width):
    segments = strike.shape[1]
    rows = lax.broadcasted_iota(jnp.int32, (segments, segments), 0)
    diagonal = rows == lax.broadcasted_iota(jnp.int32, (segments, segments), 1)
    matches = lax.broadcasted_iota(jnp.int32, (segments, ids.shape[1]), 0) == ids

    def lookup(row):
        column = jnp.sum(jnp.where(diagonal, row, 0.0), axis=1, keepdims=True)
        return jnp.sum(jnp.where(matches, column, 0.0), axis=0, keepdims=True)

    angles = jnp.concatenate([lookup(strike), lookup(dip)], axis=0)
    sines, cosines = jnp.sin(angles), jnp.cos(angles)
    table = jnp.concatenate([pos, depth, sines[0:1], cosines[0:1], sines[1:2], cosines[1:2]], axis=0)
    table = jnp.where(core == 1, table[:, width:], table[:, :width])
    table = jnp.concatenate([table, jnp.zeros((7, LANES // 4 - width), jnp.float32)], axis=1)
    spare = jnp.zeros((1, LANES // 4), jnp.float32)
    upper = jnp.concatenate([table[k : k + 1] for k in range(4)], axis=1)
    lower = jnp.concatenate([table[k : k + 1] for k in range(4, 7)] + [spare], axis=1)
    return jnp.concatenate([upper, lower], axis=0)


def kernel(
    n,
    *refs,
):
    args, refs = refs[:11], refs[11:]
    residual_ref, misfit_ref, refs = refs[0], refs[1], refs[2:]
    local, refs = refs[:11], refs[11:]
    (
        sites_own,
        sites_in,
        slips_in,
        greens,
        acc,
        part_in,
        sums_in,
        load_sem,
        line_send,
        hop_send,
        slip_recv,
        pair_send,
        pair_recv,
        sums_send,
        sums_recv,
    ) = refs
    me = lax.axis_index("patch")
    core = lax.axis_index("pix")
    line = n // 4
    count = 2 * n
    rank = me * 2 + core
    place = me // 4
    across_x = me + 1 - 2 * lax.rem(me, 2)
    across_y = me + 2 - 4 * lax.rem(me // 2, 2)
    heading = 1 - 2 * (place // (line - line // 2))
    sibling = 1 - core
    width = local[10].shape[1]
    pixels = residual_ref.shape[0]

    barrier = pltpu.get_barrier_semaphore()

    def greet(target):
        pl.semaphore_signal(barrier, inc=1, device_id=target, device_id_type=MESH)

    @pl.loop(1, line)
    def _(t):
        greet((lax.rem(me + 4 * t, n), core))

    greet((across_x, core))
    greet((across_y, core))
    greet((me, sibling))

    loads = []
    for k in range(11):
        src = args[k]
        if k == 10:
            src = src.at[:, pl.ds(pl.multiple_of(core * width, 8), width)]
        loads.append(pltpu.make_async_copy(src, local[k], load_sem.at[k]))
    for load in loads:
        load.start()
    for load in loads:
        load.wait()

    sites_own[...] = jnp.zeros_like(sites_own)
    sites_own[0:2, :pixels] = local[0][...]
    sites_own[2:5, :pixels] = local[1][...] * inv_two_pi
    frames = frame_table(core, *[local[k][...] for k in range(5, 10)], width)
    high = frames.astype(jnp.bfloat16).astype(jnp.float32)
    middle = (frames - high).astype(jnp.bfloat16).astype(jnp.float32)
    slip = local[10][...].astype(jnp.float32)
    rows = [slip[k] for k in range(3)] + [high, middle, frames - high - middle, 0.0 * high]
    slips_in[0, place] = jnp.concatenate(rows, axis=0).astype(jnp.bfloat16)

    pl.semaphore_wait(barrier, line + 2)

    def remote(src, dst, send, recv, target):
        return pltpu.make_async_remote_copy(
            src_ref=src,
            dst_ref=dst,
            send_sem=send,
            recv_sem=recv,
            device_id=target,
            device_id_type=MESH,
        )

    def line_copy(t):
        mine = slips_in.at[0, place]
        target = lax.rem(me + 4 * t, n)
        return remote(mine, mine, line_send.at[t], slip_recv.at[0, place], (target, core))

    def hop_copy(kind, quad, into, slot, target):
        return remote(
            slips_in.at[quad, slot],
            slips_in.at[into, slot],
            hop_send.at[kind, slot],
            slip_recv.at[into, slot],
            (target, core),
        )

    def side_copies(slot):
        return (hop_copy(0, 0, 1, slot, across_y), hop_copy(1, 0, 2, slot, across_x))

    def corner_copy(slot):
        odd = lax.rem(slot, 2)
        target = across_x + odd * (across_y - across_x)
        return hop_copy(2, 1 + odd, 3, slot, target)

    def wait_block(quad, slot):
        ref, sem = slips_in.at[quad, slot], slip_recv.at[quad, slot]
        remote(ref, ref, hop_send.at[0, slot], sem, (across_x, core)).wait_recv()

    def slot_at(t):
        return lax.rem(place + t * heading + line, line)

    sites_copy = remote(sites_own, sites_in, pair_send.at[0], pair_recv.at[0], (me, sibling))
    for copy in side_copies(place):
        copy.start()

    @pl.loop(1, line)
    def _(t):
        line_copy(t).start()

    sites_copy.start()

    def add_green(quad, slot):
        packed = slips_in[quad, slot, 3 * width :, :].astype(jnp.float32)
        frames = packed[0:2] + packed[2:4] + packed[4:6]
        turned = jnp.concatenate([frames, jnp.zeros((6, LANES), jnp.float32)], axis=0).T
        columns = []
        for k in range(7):
            base = (k % 4) * (LANES // 4)
            columns.append(turned[base : base + width, k // 4 : k // 4 + 1])
        for lane, ref in enumerate((sites_own, sites_in)):
            rows = green_rows(ref[...], columns) + (jnp.zeros((8, LANES), jnp.float32),)
            block = jnp.concatenate(rows, axis=0).astype(jnp.bfloat16)
            greens[quad, slot, :, lane * LANES : (lane + 1) * LANES] = block

    def turn_corner(slot):
        quad = 1 + lax.rem(slot, 2)
        wait_block(quad, slot)
        corner_copy(slot).start()
        add_green(quad, slot)

    sites_copy.wait_recv()
    add_green(0, place)

    @pl.loop(1, line)
    def _(t):
        slot = slot_at(t)
        wait_block(0, slot)
        for copy in side_copies(slot):
            copy.start()
        add_green(0, slot)
        turn_corner(slot_at(t - 1))

    turn_corner(slot_at(line - 1))

    @pl.loop(0, line)
    def _(t):
        slot = slot_at(t)
        quad = 2 - lax.rem(slot, 2)
        wait_block(quad, slot)
        add_green(quad, slot)

    chunk = math.gcd(line, 8)

    def product(side, step, lane):
        slips = slips_in[side, pl.ds(step * chunk, chunk)]
        block = greens[side, pl.ds(step * chunk, chunk), :, lane * LANES : (lane + 1) * LANES]
        return lax.dot_general(
            slips.reshape(-1, slips.shape[-1]),
            block.reshape(-1, LANES),
            (((0,), (0,)), ((), ())),
            preferred_element_type=jnp.float32,
        )

    acc[...] = jnp.zeros_like(acc)

    @pl.loop(0, line // chunk)
    def _(step):
        for lane in range(2):
            for quad in range(3):
                acc[lane] += product(quad, step, lane)

    @pl.loop(0, line)
    def _(t):
        slot = slot_at(t)
        wait_block(3, slot)
        add_green(3, slot)

    @pl.loop(0, line // chunk)
    def _(step):
        acc[1] += product(3, step, 1)

    part_copy = remote(acc.at[1], part_in, pair_send.at[1], pair_recv.at[1], (me, sibling))
    part_copy.start()

    @pl.loop(0, line // chunk)
    def _(step):
        acc[0] += product(3, step, 0)

    valid = local[4][...].astype(jnp.float32)
    part_copy.wait_recv()
    total = (acc[0] + part_in[...])[:, :pixels]
    scaled = valid * (total - local[2][...]) / local[3][...]
    blank = jnp.zeros((total.shape[0], LANES - pixels), jnp.float32)
    residual = jnp.concatenate([scaled, blank], axis=1).T[:pixels]
    sums_in[rank] = jnp.sum(residual * residual, axis=0, keepdims=True)

    def sums_copy(t, slot):
        peer = lax.rem(rank + t, count)
        return remote(
            sums_in.at[slot],
            sums_in.at[slot],
            sums_send.at[t],
            sums_recv.at[slot],
            (peer // 2, lax.rem(peer, 2)),
        )

    @pl.loop(1, count)
    def _(t):
        sums_copy(t, rank).start()

    residual_ref[...] = residual
    sites_copy.wait_send()
    part_copy.wait_send()

    @pl.loop(1, line)
    def _(t):
        line_copy(t).wait_send()

    @pl.loop(0, line)
    def _(slot):
        for copy in side_copies(slot):
            copy.wait_send()
        corner_copy(slot).wait_send()

    @pl.loop(1, count)
    def _(t):
        sums_copy(t, rank).wait_send()
        sums_copy(t, lax.rem(rank + t, count)).wait_recv()

    misfit_ref[...] = jnp.sum(sums_in[...], axis=0) / (pixels * count)


def per_device(n, *args):
    args = [arg.reshape(1, -1) if arg.ndim == 1 else arg for arg in args]
    args[10] = args[10].transpose(1, 0, 2)
    own_pixels = args[0].shape[1]
    width = args[10].shape[1] // 2
    samples = args[10].shape[2]
    line = n // 4
    vmem = pl.BlockSpec(memory_space=pltpu.VMEM)
    local = [pltpu.VMEM(arg.shape, arg.dtype) for arg in args[:10]]
    local.append(pltpu.VMEM((3, width, samples), jnp.bfloat16))
    depth = 3 * width + 8
    dma = pltpu.SemaphoreType.DMA
    residual, misfit = pl.pallas_call(
        functools.partial(kernel, n),
        out_shape=(
            pltpu.VMEM((own_pixels, samples), jnp.float32),
            pltpu.VMEM((1, samples), jnp.float32),
        ),
        in_specs=[pl.BlockSpec(memory_space=pl.ANY)] * 11,
        out_specs=(vmem, vmem),
        scratch_shapes=local
        + [
            pltpu.VMEM((8, LANES), jnp.float32),
            pltpu.VMEM((8, LANES), jnp.float32),
            pltpu.VMEM((4, line, depth, samples), jnp.bfloat16),
            pltpu.VMEM((4, line, depth, 2 * LANES), jnp.bfloat16),
            pltpu.VMEM((2, samples, LANES), jnp.float32),
            pltpu.VMEM((samples, LANES), jnp.float32),
            pltpu.VMEM((2 * n, 1, samples), jnp.float32),
            dma((11,)),
            dma((line,)),
            dma((3, line)),
            dma((4, line)),
            dma((2,)),
            dma((2,)),
            dma((2 * n,)),
            dma((2 * n,)),
        ],
        compiler_params=pltpu.CompilerParams(collective_id=0, has_side_effects=True),
    )(*args)
    return residual, misfit.reshape(samples)


def solution(mesh):
    return jax.shard_map(
        functools.partial(per_device, mesh.shape["patch"]),
        mesh=mesh,
        in_specs=(
            P(None, ("patch", "pix")),
            P(None, ("patch", "pix")),
            P(("patch", "pix")),
            P(("patch", "pix")),
            P(("patch", "pix")),
            P(None, "patch"),
            P("patch"),
            P("patch"),
            P(),
            P(),
            P("patch", None, None),
        ),
        out_specs=(P(("patch", "pix"), None), P()),
        check_vma=False,
    )
```
